32 devices in a mesh: group: 2 (over y), section: 4 (over x, core), tensor: 4 (over z).
Axes of the slice: x: 2, y: 2, z: 4, core: 2. Of those that a mesh axis runs over, the one named last changes fastest.
Arguments:
- hidden_states: bfloat16 [2, 4, 4, 8192], P('group', 'section', 'tensor'), may hold values from -6 to 6
- query_train: bfloat16 [4, 8192, 4096], P(None, ('group', 'section'), 'tensor'), may hold values from -0.0625 to 0.0625
- keyval_train: bfloat16 [4, 8192, 1024], P(None, ('group', 'section'), 'tensor'), may hold values from -0.0625 to 0.0625
- layer_of_section: int32 [4], replicated, may hold values from 0 to 3, each once
- lengths: int32 [2, 4, 4], P('group', 'section', 'tensor'), may hold values from 2 to 1024
- kv_cache: bfloat16 [2, 4, 4, 1024, 1024], P('group', 'section', 'tensor'), as said below
Outputs:
- attended: bfloat16 [2, 4, 4, 4096], P('group', 'section', 'tensor')
- new_entries: bfloat16 [2, 4, 4, 1024], P('group', 'section', 'tensor')
The draws below stay inside these ranges and needn't reach their ends.
Inputs may be any that keep to these rules, and one draw needn't show every extreme that they name: `layer_of_section`: every layer appears once. `kv_cache`: cache positions at or past a sequence's length hold entries that are never read.
All inputs are finite; a program needn't handle non-finite values.
Results may differ from the reference program's by a relative error of at most 0.03.
Values may be sent and summed in bfloat16 or wider, within the bound.
A program may use at most 64 MiB of HBM per device.

```python
import jax
import jax.numpy as jnp
from jax import lax

D = 8192
HD = 128
QH = 32
KVH = 4
KV_LEN = 1024
LAYERS = 4
BATCH = 4
N_GROUP = 2
N_SECTION = 4


def draw_kv_cache(key, part):
    shape = (N_GROUP, N_SECTION, BATCH, KV_LEN, 2 * KVH * HD)
    base = jax.random.normal(jax.random.fold_in(key, 11), shape, jnp.float32)
    return base.astype(jnp.bfloat16)


def plant(values, stream_key, least, high):
    longest = values.shape.index(max(values.shape))
    spots = []
    for shift in (0, 1):
        where = [jax.random.randint(jax.random.fold_in(stream_key, axis), (), 0, length) for axis, length in enumerate(values.shape)]
        where[longest] = (where[longest] + shift) % values.shape[longest]
        spots.append(tuple(where))
    return values.at[spots[0]].set(least).at[spots[1]].set(high)


def shard_levels(key, dims, shards, least, top_value):
    gain = 1.0
    for axis_at, parts in shards:
        heights = jax.random.uniform(jax.random.fold_in(jax.random.fold_in(key, 6), axis_at), (parts,), jnp.float32, least / len(shards), top_value / len(shards))
        gain = gain * jnp.repeat(jnp.exp(heights), dims[axis_at] // parts).reshape((-1,) + (1,) * (len(dims) - 1 - axis_at))
    return gain


def noise(stream_key, dims, width, limit, pieces=(), kind=jnp.bfloat16):
    loudness = shard_levels(stream_key, dims, pieces, -0.22, 0.18) if pieces else 1.0
    drawn = jax.random.normal(stream_key, dims, jnp.float32) * width * loudness
    return jnp.minimum(jnp.maximum(drawn, -limit), limit).astype(kind)


def setup_inputs(seed: int = 0) -> dict:
    streams_of = jax.random.split(jax.random.key(seed), 7)
    return {
        "hidden_states": noise(streams_of[0], (N_GROUP, N_SECTION, BATCH, D), 1.0, 6.0, ((0, 2), (1, 4), (2, 4))),
        "query_train": noise(streams_of[1], (LAYERS, D, QH * HD), D ** -0.5, 0.0625, ((1, 8), (2, 4))),
        "keyval_train": noise(streams_of[2], (LAYERS, D, 2 * KVH * HD), D ** -0.5, 0.0625, ((1, 8), (2, 4))),
        "layer_of_section": jax.random.permutation(streams_of[3], LAYERS).astype(jnp.int32),
        "lengths": plant(jax.random.randint(streams_of[4], (N_GROUP, N_SECTION, BATCH), 2, KV_LEN + 1), jax.random.fold_in(streams_of[4], 1), 2, KV_LEN).astype(jnp.int32),
        "kv_cache": draw_kv_cache(jax.random.fold_in(streams_of[6], 71), 0),
    }


def rotate(vectors, position):
    half_size = HD // 2
    inverse = jnp.power(jnp.float32(500000.0), -jnp.arange(half_size, dtype=jnp.float32) * 2.0 / HD)
    angle = position[:, None, None] * inverse[None, None, :]
    cosine = jnp.cos(angle)
    sine_part = jnp.sin(angle)
    first_half = vectors[..., :half_size]
    second = vectors[..., half_size:]
    return jnp.concatenate([first_half * cosine - second * sine_part, second * cosine + first_half * sine_part], axis=-1)

def attend(queries, key_value, seq_lens, cache):
    count = queries.shape[0]
    per_kv = QH // KVH
    position = seq_lens.astype(jnp.float32)
    query_rot = rotate(queries.astype(jnp.float32).reshape(count, QH, HD), position).astype(jnp.bfloat16)
    key_rot = rotate(key_value[:, :KVH * HD].astype(jnp.float32).reshape(count, KVH, HD), position).astype(jnp.bfloat16)
    new_values = key_value[:, KVH * HD:]
    cache_keys = cache[:, :, :KVH * HD].reshape(count, KV_LEN, KVH, HD).astype(jnp.float32)
    cache_values = cache[:, :, KVH * HD:].reshape(count, KV_LEN, KVH, HD).astype(jnp.float32)
    query_group = query_rot.astype(jnp.float32).reshape(count, KVH, per_kv, HD)
    score_scale = 1.0 / jnp.sqrt(jnp.float32(HD))
    scores = jnp.einsum('skgd,sjkd->skgj', query_group, cache_keys) * score_scale
    own_score = jnp.einsum('skgd,skd->skg', query_group, key_rot.astype(jnp.float32)) * score_scale
    usable = (jnp.arange(KV_LEN, dtype=jnp.int32)[None, :] < seq_lens[:, None])[:, None, None, :]
    scores = jnp.where(usable, scores, jnp.float32(-1e+30))
    largest = jnp.maximum(lax.optimization_barrier(jnp.max(scores, axis=-1)), own_score)
    exponent = jnp.where(usable, jnp.exp(scores - largest[..., None]), jnp.float32(0.0))
    own_exp = jnp.exp(own_score - largest)
    totals = lax.optimization_barrier(jnp.sum(exponent, axis=-1)) + own_exp
    probs = (exponent / totals[..., None]).astype(jnp.bfloat16)
    own_prob = (own_exp / totals).astype(jnp.bfloat16)
    new_float = new_values.astype(jnp.float32).reshape(count, KVH, HD)
    result = jnp.einsum('skgj,sjkd->skgd', probs.astype(jnp.float32), cache_values)
    result = result + own_prob.astype(jnp.float32)[..., None] * new_float[:, :, None, :]
    entries = jnp.concatenate([key_rot.reshape(count, KVH * HD), new_values], axis=1)
    return (result.reshape(count, QH * HD).astype(jnp.bfloat16), entries)

def reference(hidden_states, query_train, keyval_train, layer_of_section, lengths, kv_cache):
    pairs = N_GROUP * N_SECTION
    stacked = hidden_states.reshape(pairs, BATCH, D)
    layer_list = jnp.tile(layer_of_section.astype(jnp.int32), N_GROUP)
    len_rows = lengths.reshape(pairs, BATCH)
    cache_rows = kv_cache.reshape(pairs, BATCH, KV_LEN, 2 * KVH * HD)

    def one_pair(inputs):
        tokens, layer, seq_lens, cache = inputs
        w_query = lax.dynamic_index_in_dim(query_train, layer, 0, keepdims=False)
        w_keyval = lax.dynamic_index_in_dim(keyval_train, layer, 0, keepdims=False)
        queries = jnp.dot(tokens, w_query, preferred_element_type=jnp.float32).astype(jnp.bfloat16)
        key_value = jnp.dot(tokens, w_keyval, preferred_element_type=jnp.float32).astype(jnp.bfloat16)
        return attend(queries, key_value, seq_lens, cache)
    result, entries = lax.map(one_pair, (stacked, layer_list, len_rows, cache_rows))
    return (result.reshape(N_GROUP, N_SECTION, BATCH, QH * HD), entries.reshape(N_GROUP, N_SECTION, BATCH, 2 * KVH * HD))
```

```python
import functools

import jax
import jax.numpy as jnp
from jax import lax
from jax.experimental import pallas as pl
from jax.experimental.pallas import tpu as pltpu
from jax.sharding import PartitionSpec as P

HD = 128
MESH = pl.DeviceIdType.MESH


def kernel(sizes, layer_hbm, len_hbm, h_hbm, wq_hbm, wk_hbm, cache_hbm, out_ref, ent_ref,
           layer_ref, len_ref, h_vm, h_rows, h_pack, x_all, x_rows, wq, wk, cache, send_p, recv_p, send_z, recv_z, heads,
           sem_i, sem_h, sem_w, sem_c, a_send, a_recv, b_send, b_recv, p_send, p_recv, z_send, z_recv):
    n_group, n_section, n_tensor = sizes
    n_plane = n_group * n_section
    g, s, t = lax.axis_index("group"), lax.axis_index("section"), lax.axis_index("tensor")
    me = g * n_section + s
    rows = wq.shape[1]
    q_cols, k_cols = wq.shape[2], wk.shape[2]
    kv_heads = cache.shape[1] // 2 // HD
    q_heads = q_cols * n_tensor // HD
    per_kv = q_heads // kv_heads

    def plane_id(p):
        return (p // n_section, lax.rem(p, n_section), t)

    barrier = pltpu.get_barrier_semaphore()
    plane = [lax.rem(me + k, n_plane) for k in range(1, n_plane)]
    line = [lax.rem(t + k, n_tensor) for k in range(1, n_tensor)]
    for p in plane:
        pl.semaphore_signal(barrier, inc=1, device_id=plane_id(p), device_id_type=MESH)
    for z in line:
        pl.semaphore_signal(barrier, inc=1, device_id=(g, s, z), device_id_type=MESH)

    load_h = pltpu.make_async_copy(h_hbm, h_vm, sem_h)
    load_h.start()
    load_layer = pltpu.make_async_copy(layer_hbm, layer_ref, sem_i.at[0])
    load_len = pltpu.make_async_copy(len_hbm, len_ref, sem_i.at[1])
    load_layer.start()
    load_len.start()
    loads = []
    for l in range(n_section):
        loads.append(pltpu.make_async_copy(wq_hbm.at[l], wq.at[l], sem_w.at[0, l]))
        loads.append(pltpu.make_async_copy(wk_hbm.at[l], wk.at[l], sem_w.at[1, l]))
    load_c = pltpu.make_async_copy(cache_hbm, cache, sem_c)
    for c in loads:
        c.start()
    load_c.start()

    tile = rows // HD
    load_h.wait()
    for j in range(n_plane * tile):
        h_rows[j:j + 1, :] = h_vm[:, j * HD:(j + 1) * HD].astype(jnp.float32)
    for p in range(n_plane):
        h_pack[p] = h_rows[p * tile:(p + 1) * tile, :].astype(jnp.bfloat16)
    x_all[t, me] = h_pack[me]
    load_layer.wait()
    load_len.wait()
    pl.semaphore_wait(barrier, n_plane - 1 + n_tensor - 1)

    def copy_a(p, slot, sem):
        return pltpu.make_async_remote_copy(
            src_ref=h_pack.at[p],
            dst_ref=x_all.at[t, slot],
            send_sem=a_send.at[p], recv_sem=a_recv.at[sem],
            device_id=plane_id(p), device_id_type=MESH)

    for p in plane:
        copy_a(p, me, me).start()

    half = HD // 2
    lane = lax.broadcasted_iota(jnp.int32, (1, HD), 1)
    freq_at = jnp.where(lane < half, lane, lane - half).astype(jnp.float32)
    inverse = jnp.exp(freq_at * jnp.float32(-2.0 / HD) * jnp.log(jnp.float32(500000.0)))
    seq_len = len_ref[0, 0, 0]
    angle = seq_len.astype(jnp.float32) * inverse
    cosine = jnp.cos(angle)
    sine = jnp.where(lane < half, -jnp.sin(angle), jnp.sin(angle))

    for p in plane:
        copy_a(p, p, p).wait_recv()

    def copy_b(z, slot, sem):
        return pltpu.make_async_remote_copy(
            src_ref=x_all.at[t], dst_ref=x_all.at[slot],
            send_sem=b_send.at[z], recv_sem=b_recv.at[sem],
            device_id=(g, s, z), device_id_type=MESH)

    for z in line:
        copy_b(z, t, t).start()

    def place(b):
        for gg in range(n_group):
            for ss in range(n_section):
                at = pl.multiple_of((gg * n_tensor + b) * tile, tile)
                x_rows[ss, pl.ds(at, tile), :] = x_all[b, gg * n_section + ss].astype(jnp.float32)

    place(t)
    for c in loads:
        c.wait()
    for z in line:
        copy_b(z, z, z).wait_recv()
        place(z)

    base = (s // 2) * 2 + 2

    def copy_p(p, slot, sem):
        return pltpu.make_async_remote_copy(
            src_ref=send_p.at[p], dst_ref=recv_p.at[slot],
            send_sem=p_send.at[p], recv_sem=p_recv.at[sem],
            device_id=plane_id(p), device_id_type=MESH)

    def section_step(k, carry):
        ss = lax.rem(base + k, n_section)
        layer = layer_ref[ss]
        tokens = jnp.concatenate(
            [x_rows[ss, pl.ds(i, n_group * n_tensor, stride=tile), :] for i in range(tile)],
            axis=1).astype(jnp.bfloat16)
        part_q = jnp.dot(tokens, wq[layer], preferred_element_type=jnp.float32)
        part_k = jnp.dot(tokens, wk[layer], preferred_element_type=jnp.float32)
        for gg in range(n_group):
            p = gg * n_section + ss
            lo, hi = gg * n_tensor, (gg + 1) * n_tensor
            send_p[p, :, 0:q_cols] = part_q[lo:hi].astype(send_p.dtype)
            send_p[p, :, q_cols:q_cols + k_cols] = part_k[lo:hi].astype(send_p.dtype)

            @pl.when(p != me)
            def _():
                copy_p(p, me, me).start()
        return carry

    lax.fori_loop(0, n_section, section_step, 0)

    total = send_p[me].astype(jnp.float32)
    for p in plane:
        copy_p(p, p, p).wait_recv()
        total += recv_p[p].astype(jnp.float32)

    def copy_z(z, slot, sem):
        return pltpu.make_async_remote_copy(
            src_ref=send_z.at[z], dst_ref=recv_z.at[slot],
            send_sem=z_send.at[z], recv_sem=z_recv.at[sem],
            device_id=(g, s, z), device_id_type=MESH)

    for b in range(n_tensor):
        send_z[b] = total[b:b + 1].astype(jnp.bfloat16)
    for z in line:
        copy_z(z, t, t).start()

    q_per, k_per = q_cols // HD, k_cols // HD

    def spread(src, z):
        row = src.astype(jnp.float32)
        for j in range(q_per):
            heads[pl.ds(z * q_per + j, 1), :] = row[:, j * HD:(j + 1) * HD]
        for j in range(k_per):
            heads[pl.ds(q_heads + z * k_per + j, 1), :] = row[:, q_cols + j * HD:q_cols + (j + 1) * HD]

    spread(send_z[t], t)
    for z in line:
        copy_z(z, z, z).wait_recv()
        spread(recv_z[z], z)
    if k_per == 0:
        for z in range(n_tensor):
            row = jnp.where(t == z, send_z[z], recv_z[z]).astype(jnp.float32)
            at, lo = divmod(z * k_cols, HD)
            heads[q_heads + at:q_heads + at + 1, lo:lo + k_cols] = row[:, q_cols:q_cols + k_cols]

    def rotate(u):
        return (u * cosine + pltpu.roll(u, half, 1) * sine).astype(jnp.bfloat16)

    query_rot = rotate(heads[0:q_heads])
    key_rot = rotate(heads[q_heads:q_heads + kv_heads])
    new_value = heads[q_heads + kv_heads:q_heads + 2 * kv_heads]
    for j in range(kv_heads):
        ent_ref[0, 0, :, j * HD:(j + 1) * HD] = key_rot[j:j + 1].astype(jnp.float32).astype(jnp.bfloat16)
        at = (kv_heads + j) * HD
        ent_ref[0, 0, :, at:at + HD] = new_value[j:j + 1].astype(jnp.bfloat16)

    def per_query(u):
        return jnp.concatenate(
            [jnp.broadcast_to(u[k:k + 1], (per_kv, HD)) for k in range(kv_heads)], axis=0)

    scale = 1.0 / jnp.sqrt(jnp.float32(HD))
    query_float = query_rot.astype(jnp.float32)
    own_score = jnp.sum(query_float * per_query(key_rot.astype(jnp.float32)), axis=1, keepdims=True) * scale
    head_row = lax.broadcasted_iota(jnp.int32, (q_heads, HD), 0) // per_kv
    wide = jnp.concatenate(
        [jnp.where(head_row == k, query_float, 0.0) for k in range(kv_heads)], axis=1).astype(jnp.bfloat16)
    load_c.wait()
    kv_cols = kv_heads * HD
    scores = lax.dot_general(wide, cache[:, 0:kv_cols], (((1,), (1,)), ((), ())),
                             preferred_element_type=jnp.float32) * scale
    usable = lax.broadcasted_iota(jnp.int32, scores.shape, 1) < seq_len
    scores = jnp.where(usable, scores, jnp.float32(-1e30))
    largest = jnp.maximum(jnp.max(scores, axis=1, keepdims=True), own_score)
    exponent = jnp.where(usable, jnp.exp(scores - largest), 0.0)
    own_exp = jnp.exp(own_score - largest)
    inv_total = 1.0 / (jnp.sum(exponent, axis=1, keepdims=True) + own_exp)
    probs = (exponent * inv_total).astype(jnp.bfloat16)
    own_prob = (own_exp * inv_total).astype(jnp.bfloat16).astype(jnp.float32)
    mixed = jnp.dot(probs, cache[:, kv_cols:2 * kv_cols], preferred_element_type=jnp.float32)
    picked = jnp.concatenate(
        [mixed[k * per_kv:(k + 1) * per_kv, k * HD:(k + 1) * HD] for k in range(kv_heads)], axis=0)
    attended = picked + own_prob * per_query(new_value)
    for j in range(q_heads):
        out_ref[0, 0, :, j * HD:(j + 1) * HD] = attended[j:j + 1].astype(jnp.bfloat16)

    for p in plane:
        copy_a(p, me, me).wait_send()
        copy_p(p, me, me).wait_send()
    for z in line:
        copy_b(z, t, t).wait_send()
        copy_z(z, t, t).wait_send()


def shards(sizes, hidden_states, query_train, keyval_train, layer_of_section, lengths, kv_cache):
    n_group, n_section, n_tensor = sizes
    n_plane = n_group * n_section
    d = hidden_states.shape[-1]
    layers, rows, q_cols = query_train.shape
    k_cols = keyval_train.shape[2]
    kv_len, kv_width = kv_cache.shape[-2:]
    q_heads = q_cols * n_tensor // HD
    kv2 = kv_width // HD
    bf16 = jnp.bfloat16
    hbm = pl.BlockSpec(memory_space=pltpu.HBM)
    anym = pl.BlockSpec(memory_space=pl.ANY)
    vmem = pl.BlockSpec(memory_space=pltpu.VMEM)
    dma = pltpu.SemaphoreType.DMA
    return pl.pallas_call(
        functools.partial(kernel, sizes),
        out_shape=(pltpu.VMEM((1, 1, 1, q_heads * HD), bf16), pltpu.VMEM((1, 1, 1, kv_width), bf16)),
        in_specs=[hbm, hbm, anym, anym, anym, anym],
        out_specs=(vmem, vmem),
        scratch_shapes=[
            pltpu.SMEM(layer_of_section.shape, jnp.int32),
            pltpu.SMEM(lengths.shape, jnp.int32),
            pltpu.VMEM((1, d), bf16),
            pltpu.VMEM((d // HD, HD), jnp.float32),
            pltpu.VMEM((n_plane, rows // HD, HD), bf16),
            pltpu.VMEM((n_tensor, n_plane, rows // HD, HD), bf16),
            pltpu.VMEM((n_section, n_group * n_tensor * (rows // HD), HD), jnp.float32),
            pltpu.VMEM((layers, rows, q_cols), bf16),
            pltpu.VMEM((layers, rows, k_cols), bf16),
            pltpu.VMEM((kv_len, kv_width), bf16),
            pltpu.VMEM((n_plane, n_tensor, q_cols + k_cols), bf16),
            pltpu.VMEM((n_plane, n_tensor, q_cols + k_cols), bf16),
            pltpu.VMEM((n_tensor, 1, q_cols + k_cols), bf16),
            pltpu.VMEM((n_tensor, 1, q_cols + k_cols), bf16),
            pltpu.VMEM((q_heads + kv2, HD), jnp.float32),
            dma((2,)), dma, dma((2, layers)), dma,
            dma((n_plane,)), dma((n_plane,)), dma((n_tensor,)), dma((n_tensor,)),
            dma((n_plane,)), dma((n_plane,)), dma((n_tensor,)), dma((n_tensor,)),
        ],
        compiler_params=pltpu.CompilerParams(collective_id=0, has_side_effects=True),
    )(layer_of_section, lengths, hidden_states.reshape(1, d), query_train, keyval_train,
      kv_cache.reshape(kv_len, kv_width))


def solution(mesh):
    sizes = (mesh.shape["group"], mesh.shape["section"], mesh.shape["tensor"])
    in_specs = (
        P("group", "section", "tensor", None),
        P(None, ("group", "section"), "tensor"),
        P(None, ("group", "section"), "tensor"),
        P(),
        P("group", "section", "tensor"),
        P("group", "section", "tensor", None, None),
    )
    out_specs = (P("group", "section", "tensor", None), P("group", "section", "tensor", None))
    return jax.shard_map(
        functools.partial(shards, sizes), mesh=mesh, in_specs=in_specs, out_specs=out_specs, check_vma=False)
```
